32 devices in a mesh: lat: 4 (over z), lon: 4 (over y, x), lev: 2 (over core).
Axes of the slice: x: 2, y: 2, z: 4, core: 2. Of those that a mesh axis runs over, the one named last changes fastest.
Arguments:
- pressure: float32 [16, 256, 128, 128], P('lat', 'lon', 'lev'), may hold values from 0.2 to 1.8
- earlier: float32 [16, 256, 128, 128], P('lat', 'lon', 'lev'), may hold values from 0.2 to 1.8
- speed_square: float32 [16, 256, 128, 128], P('lat', 'lon', 'lev'), may hold values from 0.05 to 0.3
Outputs:
- pressure_end: float32 [16, 256, 128, 128], P('lat', 'lon', 'lev')
The draws below stay inside these ranges and needn't reach their ends.
All inputs are finite; a program needn't handle non-finite values.
Results may differ from the reference program's by a relative error of at most 0.00002.
Values sent between devices are 32-bit elements.
A program may use at most 320 MiB of HBM per device.

```python
import jax
import jax.numpy as jnp
from jax import lax

GRID_Y = 16
GRID_X = 256
GRID_Z = 128
LEVELS = 128
STEPS = 4


def block_levels(stream_key, extent, cuts, least, high):
    def one(dim, shards_of):
        steps = jax.random.uniform(jax.random.fold_in(jax.random.fold_in(stream_key, 6), dim), (shards_of,), jnp.float32, least / len(cuts), high / len(cuts))
        return jnp.repeat(jnp.exp(steps), extent[dim] // shards_of).reshape((-1,) + (1,) * (len(extent) - dim - 1))

    factor_of = one(*cuts[0])
    for cut in cuts[1:]:
        factor_of = factor_of * one(*cut)
    return factor_of


def setup_inputs(seed: int = 0) -> dict:
    splits = jax.random.split(jax.random.key(seed), 4)
    return {
        "pressure": jnp.clip(0.2 + 1.5999999 * jax.random.uniform(splits[0], (GRID_Y, GRID_X, GRID_Z, LEVELS), jnp.float32) ** block_levels(splits[0], (GRID_Y, GRID_X, GRID_Z, LEVELS), ((0, 4), (1, 4), (2, 2)), -0.2, 0.2), 0.2, 1.8),
        "earlier": jnp.clip(0.2 + 1.5999999 * jax.random.uniform(splits[1], (GRID_Y, GRID_X, GRID_Z, LEVELS), jnp.float32) ** block_levels(splits[1], (GRID_Y, GRID_X, GRID_Z, LEVELS), ((0, 4), (1, 4), (2, 2)), -0.2, 0.2), 0.2, 1.8),
        "speed_square": jnp.clip(0.05 + 0.25 * jax.random.uniform(splits[2], (GRID_Y, GRID_X, GRID_Z, LEVELS), jnp.float32) ** block_levels(splits[2], (GRID_Y, GRID_X, GRID_Z, LEVELS), ((0, 4), (1, 4), (2, 2)), -0.2, 0.2), 0.05, 0.3),
    }


def inner_cells(values, dims):
    for dim in dims:
        values = lax.slice_in_dim(values, 1, values.shape[dim] - 1, axis=dim)
    return values


def side_cells(values, dim, start, dims):
    others = [other for other in dims if other != dim]
    values = inner_cells(values, others)
    return lax.slice_in_dim(values, start, start + values.shape[dim] - 2, axis=dim)


def advance(padded, before, speed_square):
    middle = inner_cells(padded, (0, 1, 2))
    lower = [side_cells(padded, dim, 0, (0, 1, 2)) for dim in (0, 1, 2)]
    upper = [side_cells(padded, dim, 2, (0, 1, 2)) for dim in (0, 1, 2)]
    spread = lower[0] + upper[0] + lower[1] + upper[1] + lower[2] + upper[2] - 6.0 * middle
    return 2.0 * middle - before + speed_square * spread


def reference(pressure, earlier, speed_square):
    for step in range(STEPS):
        later = advance(jnp.pad(pressure, ((1, 1), (1, 1), (1, 1), (0, 0)), mode="constant"), earlier, speed_square)
        earlier, pressure = pressure, later
    return pressure
```

```python
import functools
import math

import jax
import jax.numpy as jnp
from jax import lax
from jax.experimental import pallas as pl
from jax.experimental.pallas import tpu as pltpu
from jax.sharding import PartitionSpec as P

STEPS = 4
CHUNKS = 8
PAD = 8
AXES = ("lat", "lon", "lev")
MESH = pl.DeviceIdType.MESH


def kernel(
    counts,
    chunks,
    start_ref,
    earlier_ref,
    speed_ref,
    end_ref,
    even,
    odd,
    speed,
    load_sem,
    lat_send,
    lat_recv,
    side_send,
    side_recv,
):
    rows, columns, depth, lanes = start_ref.shape
    width = columns // chunks
    fields = (even, odd)
    me = [lax.axis_index(axis) for axis in AXES]
    inside = pl.ds(PAD, depth)
    below = [place > 0 for place in me]
    above = [place < count - 1 for place, count in zip(me, counts)]
    has = [(below[dim], above[dim]) for dim in range(3)]

    loads = [
        pltpu.make_async_copy(start_ref, even.at[pl.ds(1, rows), pl.ds(1, columns), inside], load_sem.at[0]),
        pltpu.make_async_copy(earlier_ref, odd.at[pl.ds(1, rows), pl.ds(1, columns), inside], load_sem.at[1]),
        pltpu.make_async_copy(speed_ref, speed, load_sem.at[2]),
    ]

    barrier = pltpu.get_barrier_semaphore()
    greeted = jnp.int32(0)
    for dim, axis in enumerate(AXES):
        for side, shift in enumerate((-1, 1)):
            greeted = greeted + has[dim][side].astype(jnp.int32)

            @pl.when(has[dim][side])
            def _():
                pl.semaphore_signal(barrier, inc=1, device_id={axis: me[dim] + shift}, device_id_type=MESH)

    pl.semaphore_wait(barrier, greeted)

    def lat_copy(step, side, chunk, target):
        field = fields[step % 2]
        first = chunk * width
        if step == 0:
            source = start_ref.at[(0, rows - 1)[side], pl.ds(first, width)]
        else:
            source = field.at[(1, rows)[side], pl.ds(first + 1, width), inside]
        return pltpu.make_async_remote_copy(
            src_ref=source,
            dst_ref=field.at[(rows + 1, 0)[side], pl.ds(first + 1, width), inside],
            send_sem=lat_send.at[step % 2, side, chunk],
            recv_sem=lat_recv.at[step % 2, side, chunk],
            device_id={"lat": target},
            device_id_type=MESH,
        )

    def side_copy(step, dim, side, target):
        field = fields[step % 2]
        if dim == 1:
            if step == 0:
                source = start_ref.at[:, (0, columns - 1)[side]]
            else:
                source = field.at[pl.ds(1, rows), (1, columns)[side], inside]
            dest = field.at[pl.ds(1, rows), (columns + 1, 0)[side], inside]
        else:
            if step == 0:
                source = start_ref.at[:, :, pl.ds((0, depth - PAD)[side], PAD)]
            else:
                source = field.at[pl.ds(1, rows), pl.ds(1, columns), pl.ds((PAD, depth)[side], PAD)]
            dest = field.at[pl.ds(1, rows), pl.ds(1, columns), pl.ds((PAD + depth, 0)[side], PAD)]
        return pltpu.make_async_remote_copy(
            src_ref=source,
            dst_ref=dest,
            send_sem=side_send.at[step % 2, dim - 1, side],
            recv_sem=side_recv.at[step % 2, dim - 1, side],
            device_id={AXES[dim]: target},
            device_id_type=MESH,
        )

    def lat_each(step, chunk, act):
        for side, shift in enumerate((-1, 1)):
            incoming = act == "recv"

            @pl.when(has[0][1 - side if incoming else side])
            def _():
                copy = lat_copy(step, side, chunk, me[0] - shift if incoming else me[0] + shift)
                if incoming:
                    copy.wait_recv()
                elif act == "send":
                    copy.wait_send()
                else:
                    copy.start()

    def side_each(step, act):
        for dim in (1, 2):
            for side, shift in enumerate((-1, 1)):
                incoming = act == "recv"

                @pl.when(has[dim][1 - side if incoming else side])
                def _():
                    copy = side_copy(step, dim, side, me[dim] - shift if incoming else me[dim] + shift)
                    if incoming:
                        copy.wait_recv()
                    elif act == "send":
                        copy.wait_send()
                    else:
                        copy.start()

    @pl.loop(0, chunks)
    def _(chunk):
        lat_each(0, chunk, "start")

    side_each(0, "start")
    for load in loads:
        load.start()

    for side in (0, 1):

        @pl.when(jnp.logical_not(has[0][side]))
        def _():
            @pl.loop(1, columns + 1)
            def _(x):
                for field in fields:
                    field[(0, rows + 1)[side], x, inside] = jnp.zeros((depth, lanes), jnp.float32)

        @pl.when(jnp.logical_not(has[1][side]))
        def _():
            for field in fields:
                for y in range(1, rows + 1):
                    field[y, (0, columns + 1)[side], inside] = jnp.zeros((depth, lanes), jnp.float32)

        @pl.when(jnp.logical_not(has[2][side]))
        def _():
            @pl.loop(1, columns + 1)
            def _(x):
                for field in fields:
                    for y in range(1, rows + 1):
                        field[y, x, pl.ds((0, PAD + depth)[side], PAD)] = jnp.zeros((PAD, lanes), jnp.float32)

    for load in loads:
        load.wait()

    outer = (1, rows) if rows > 1 else (1,)
    inner = tuple(range(2, rows))

    for step in range(STEPS):
        now, other = fields[step % 2], fields[(step + 1) % 2]
        last = step == STEPS - 1
        side_each(step, "recv")
        if step > 0:
            side_each(step - 1, "send")

        def advance(y, x):
            middle = now[y, x, inside]
            spread = (
                now[y - 1, x, inside]
                + now[y + 1, x, inside]
                + now[y, x - 1, inside]
                + now[y, x + 1, inside]
                + now[y, x, pl.ds(PAD - 1, depth)]
                + now[y, x, pl.ds(PAD + 1, depth)]
                - 6.0 * middle
            )
            later = 2.0 * middle - other[y, x, inside] + speed[y - 1, x - 1] * spread
            if last:
                end_ref[y - 1, x - 1] = later
            else:
                other[y, x, inside] = later

        @pl.loop(0, chunks)
        def _(chunk):
            lat_each(step, chunk, "recv")
            if step > 0:
                lat_each(step - 1, chunk, "send")
            for planes in (outer, inner):
                if planes:

                    @pl.loop(0, width)
                    def _(offset):
                        for y in planes:
                            advance(y, chunk * width + offset + 1)

            if not last:
                lat_each(step + 1, chunk, "start")

        if not last:
            side_each(step + 1, "start")

    side_each(STEPS - 1, "send")

    @pl.loop(0, chunks)
    def _(chunk):
        lat_each(STEPS - 1, chunk, "send")


def solution(mesh):
    counts = tuple(mesh.shape[axis] for axis in AXES)

    def shards(pressure, earlier, speed_square):
        rows, columns, depth, lanes = pressure.shape
        chunks = math.gcd(columns, CHUNKS)
        field = pltpu.VMEM((rows + 2, columns + 2, depth + 2 * PAD, lanes), jnp.float32)
        return pl.pallas_call(
            functools.partial(kernel, counts, chunks),
            out_shape=pltpu.VMEM(pressure.shape, jnp.float32),
            in_specs=[pl.BlockSpec(memory_space=pltpu.HBM)] * 3,
            out_specs=pl.BlockSpec(memory_space=pltpu.VMEM),
            scratch_shapes=[
                field,
                field,
                pltpu.VMEM(pressure.shape, jnp.float32),
                pltpu.SemaphoreType.DMA((3,)),
                pltpu.SemaphoreType.DMA((2, 2, chunks)),
                pltpu.SemaphoreType.DMA((2, 2, chunks)),
                pltpu.SemaphoreType.DMA((2, 2, 2)),
                pltpu.SemaphoreType.DMA((2, 2, 2)),
            ],
            compiler_params=pltpu.CompilerParams(
                collective_id=0, has_side_effects=True, vmem_limit_bytes=44 * 2**20
            ),
        )(pressure, earlier, speed_square)

    spec = P("lat", "lon", "lev", None)
    return jax.shard_map(
        shards, mesh=mesh, in_specs=(spec, spec, spec), out_specs=spec, check_vma=False
    )
```

```python
import functools
import math

import jax
import jax.numpy as jnp
from jax import lax
from jax.experimental import pallas as pl
from jax.experimental.pallas import tpu as pltpu
from jax.sharding import PartitionSpec as P

STEPS = 4
CHUNKS = 16
PAD = 8
AXES = ("lat", "lon", "lev")
MESH = pl.DeviceIdType.MESH


def kernel(
    counts,
    chunks,
    start_ref,
    earlier_ref,
    speed_ref,
    end_ref,
    even,
    odd,
    speed,
    load_sem,
    lat_send,
    lat_recv,
    side_send,
    side_recv,
):
    rows, columns, depth, lanes = start_ref.shape
    width = columns // chunks
    fields = (even, odd)
    me = [lax.axis_index(axis) for axis in AXES]
    inside = pl.ds(PAD, depth)
    below = [place > 0 for place in me]
    above = [place < count - 1 for place, count in zip(me, counts)]
    has = [(below[dim], above[dim]) for dim in range(3)]

    edges = (0, rows - 1) if rows > 1 else (0,)
    early = [
        pltpu.make_async_copy(
            start_ref.at[plane, pl.ds(0, width)], even.at[plane + 1, pl.ds(1, width), inside], load_sem.at[place]
        )
        for place, plane in enumerate(edges)
    ]
    loads = [
        pltpu.make_async_copy(earlier_ref, odd.at[pl.ds(1, rows), pl.ds(1, columns), inside], load_sem.at[2]),
        pltpu.make_async_copy(speed_ref, speed, load_sem.at[3]),
    ]
    if chunks > 1:
        loads += [
            pltpu.make_async_copy(
                start_ref.at[plane, pl.ds(width, columns - width)],
                even.at[plane + 1, pl.ds(1 + width, columns - width), inside],
                load_sem.at[4 + place],
            )
            for place, plane in enumerate(edges)
        ]
    if rows > 2:
        loads.append(
            pltpu.make_async_copy(
                start_ref.at[pl.ds(1, rows - 2)],
                even.at[pl.ds(2, rows - 2), pl.ds(1, columns), inside],
                load_sem.at[6],
            )
        )
    for load in early:
        load.start()

    barrier = pltpu.get_barrier_semaphore()
    greeted = jnp.int32(0)
    for dim, axis in enumerate(AXES):
        for side, shift in enumerate((-1, 1)):
            greeted = greeted + has[dim][side].astype(jnp.int32)

            @pl.when(has[dim][side])
            def _():
                pl.semaphore_signal(barrier, inc=1, device_id={axis: me[dim] + shift}, device_id_type=MESH)

    pl.semaphore_wait(barrier, greeted)

    def lat_copy(step, side, chunk, target, held):
        field = fields[step % 2]
        first = chunk * width
        if step == 0 and not held:
            source = start_ref.at[(0, rows - 1)[side], pl.ds(first, width)]
        else:
            source = field.at[(1, rows)[side], pl.ds(first + 1, width), inside]
        return pltpu.make_async_remote_copy(
            src_ref=source,
            dst_ref=field.at[(rows + 1, 0)[side], pl.ds(first + 1, width), inside],
            send_sem=lat_send.at[step % 2, side, chunk],
            recv_sem=lat_recv.at[step % 2, side, chunk],
            device_id={"lat": target},
            device_id_type=MESH,
        )

    def side_copy(step, dim, side, target):
        field = fields[step % 2]
        if dim == 1:
            if step == 0:
                source = start_ref.at[:, (0, columns - 1)[side]]
            else:
                source = field.at[pl.ds(1, rows), (1, columns)[side], inside]
            dest = field.at[pl.ds(1, rows), (columns + 1, 0)[side], inside]
        else:
            if step == 0:
                source = start_ref.at[:, :, pl.ds((0, depth - PAD)[side], PAD)]
            else:
                source = field.at[pl.ds(1, rows), pl.ds(1, columns), pl.ds((PAD, depth)[side], PAD)]
            dest = field.at[pl.ds(1, rows), pl.ds(1, columns), pl.ds((PAD + depth, 0)[side], PAD)]
        return pltpu.make_async_remote_copy(
            src_ref=source,
            dst_ref=dest,
            send_sem=side_send.at[step % 2, dim - 1, side],
            recv_sem=side_recv.at[step % 2, dim - 1, side],
            device_id={AXES[dim]: target},
            device_id_type=MESH,
        )

    def lat_each(step, chunk, act, held=False):
        for side, shift in enumerate((-1, 1)):
            incoming = act == "recv"

            @pl.when(has[0][1 - side if incoming else side])
            def _():
                copy = lat_copy(step, side, chunk, me[0] - shift if incoming else me[0] + shift, held)
                if incoming:
                    copy.wait_recv()
                elif act == "send":
                    copy.wait_send()
                else:
                    copy.start()

    def side_each(step, act):
        for dim in (1, 2):
            for side, shift in enumerate((-1, 1)):
                incoming = act == "recv"

                @pl.when(has[dim][1 - side if incoming else side])
                def _():
                    copy = side_copy(step, dim, side, me[dim] - shift if incoming else me[dim] + shift)
                    if incoming:
                        copy.wait_recv()
                    elif act == "send":
                        copy.wait_send()
                    else:
                        copy.start()

    for load in early:
        load.wait()
    lat_each(0, 0, "start", held=True)

    @pl.loop(1, chunks)
    def _(chunk):
        lat_each(0, chunk, "start")

    side_each(0, "start")
    for load in loads:
        load.start()

    for side in (0, 1):

        @pl.when(jnp.logical_not(has[0][side]))
        def _():
            @pl.loop(1, columns + 1)
            def _(x):
                for field in fields:
                    field[(0, rows + 1)[side], x, inside] = jnp.zeros((depth, lanes), jnp.float32)

        @pl.when(jnp.logical_not(has[1][side]))
        def _():
            for field in fields:
                for y in range(1, rows + 1):
                    field[y, (0, columns + 1)[side], inside] = jnp.zeros((depth, lanes), jnp.float32)

        @pl.when(jnp.logical_not(has[2][side]))
        def _():
            @pl.loop(1, columns + 1)
            def _(x):
                for field in fields:
                    for y in range(1, rows + 1):
                        field[y, x, pl.ds((0, PAD + depth)[side], PAD)] = jnp.zeros((PAD, lanes), jnp.float32)

    for load in loads:
        load.wait()

    outer = (1, rows) if rows > 1 else (1,)
    inner = tuple(range(2, rows))

    for step in range(STEPS):
        now, other = fields[step % 2], fields[(step + 1) % 2]
        last = step == STEPS - 1
        side_each(step, "recv")
        if step > 0:
            side_each(step - 1, "send")

        def advance(y, x):
            middle = now[y, x, inside]
            spread = (
                now[y - 1, x, inside]
                + now[y + 1, x, inside]
                + now[y, x - 1, inside]
                + now[y, x + 1, inside]
                + now[y, x, pl.ds(PAD - 1, depth)]
                + now[y, x, pl.ds(PAD + 1, depth)]
                - 6.0 * middle
            )
            later = 2.0 * middle - other[y, x, inside] + speed[y - 1, x - 1] * spread
            if last:
                end_ref[y - 1, x - 1] = later
            else:
                other[y, x, inside] = later

        @pl.loop(0, chunks)
        def _(chunk):
            def compute(planes):
                if planes:

                    @pl.loop(0, width)
                    def _(offset):
                        for y in planes:
                            advance(y, chunk * width + offset + 1)

            if last:
                compute(inner)
            lat_each(step, chunk, "recv")
            if step > 0:
                lat_each(step - 1, chunk, "send")
            compute(outer)
            if not last:
                compute(inner)
            if not last:
                lat_each(step + 1, chunk, "start")

        if not last:
            side_each(step + 1, "start")

    side_each(STEPS - 1, "send")

    @pl.loop(0, chunks)
    def _(chunk):
        lat_each(STEPS - 1, chunk, "send")


def solution(mesh):
    counts = tuple(mesh.shape[axis] for axis in AXES)

    def shards(pressure, earlier, speed_square):
        rows, columns, depth, lanes = pressure.shape
        chunks = math.gcd(columns, CHUNKS)
        field = pltpu.VMEM((rows + 2, columns + 2, depth + 2 * PAD, lanes), jnp.float32)
        return pl.pallas_call(
            functools.partial(kernel, counts, chunks),
            out_shape=pltpu.VMEM(pressure.shape, jnp.float32),
            in_specs=[pl.BlockSpec(memory_space=pltpu.HBM)] * 3,
            out_specs=pl.BlockSpec(memory_space=pltpu.VMEM),
            scratch_shapes=[
                field,
                field,
                pltpu.VMEM(pressure.shape, jnp.float32),
                pltpu.SemaphoreType.DMA((7,)),
                pltpu.SemaphoreType.DMA((2, 2, chunks)),
                pltpu.SemaphoreType.DMA((2, 2, chunks)),
                pltpu.SemaphoreType.DMA((2, 2, 2)),
                pltpu.SemaphoreType.DMA((2, 2, 2)),
            ],
            compiler_params=pltpu.CompilerParams(
                collective_id=0, has_side_effects=True, vmem_limit_bytes=44 * 2**20
            ),
        )(pressure, earlier, speed_square)

    spec = P("lat", "lon", "lev", None)
    return jax.shard_map(
        shards, mesh=mesh, in_specs=(spec, spec, spec), out_specs=spec, check_vma=False
    )
```

```python
import functools
import math

import jax
import jax.numpy as jnp
from jax import lax
from jax.experimental import pallas as pl
from jax.experimental.pallas import tpu as pltpu
from jax.sharding import PartitionSpec as P

STEPS = 4
CHUNKS = 8
PAD = 8
AXES = ("lat", "lon", "lev")
MESH = pl.DeviceIdType.MESH


def kernel(
    counts,
    chunks,
    start_ref,
    earlier_ref,
    speed_ref,
    end_ref,
    even,
    odd,
    speed,
    load_sem,
    lat_send,
    lat_recv,
    side_send,
    side_recv,
):
    rows, columns, depth, lanes = start_ref.shape
    width = columns // chunks
    fields = (even, odd)
    me = [lax.axis_index(axis) for axis in AXES]
    inside = pl.ds(PAD, depth)
    below = [place > 0 for place in me]
    above = [place < count - 1 for place, count in zip(me, counts)]
    has = [(below[dim], above[dim]) for dim in range(3)]

    edges = (0, rows - 1) if rows > 1 else (0,)
    early = [
        pltpu.make_async_copy(
            start_ref.at[plane, pl.ds(0, width)], even.at[plane + 1, pl.ds(1, width), inside], load_sem.at[place]
        )
        for place, plane in enumerate(edges)
    ]
    loads = [
        pltpu.make_async_copy(earlier_ref, odd.at[pl.ds(1, rows), pl.ds(1, columns), inside], load_sem.at[2]),
        pltpu.make_async_copy(speed_ref, speed, load_sem.at[3]),
    ]
    if chunks > 1:
        loads += [
            pltpu.make_async_copy(
                start_ref.at[plane, pl.ds(width, columns - width)],
                even.at[plane + 1, pl.ds(1 + width, columns - width), inside],
                load_sem.at[4 + place],
            )
            for place, plane in enumerate(edges)
        ]
    if rows > 2:
        loads.append(
            pltpu.make_async_copy(
                start_ref.at[pl.ds(1, rows - 2)],
                even.at[pl.ds(2, rows - 2), pl.ds(1, columns), inside],
                load_sem.at[6],
            )
        )
    for load in early:
        load.start()

    barrier = pltpu.get_barrier_semaphore()
    greeted = jnp.int32(0)
    for dim, axis in enumerate(AXES):
        for side, shift in enumerate((-1, 1)):
            greeted = greeted + has[dim][side].astype(jnp.int32)

            @pl.when(has[dim][side])
            def _():
                pl.semaphore_signal(barrier, inc=1, device_id={axis: me[dim] + shift}, device_id_type=MESH)

    pl.semaphore_wait(barrier, greeted)

    def lat_copy(step, side, chunk, target, held):
        field = fields[step % 2]
        first = chunk * width
        if step == 0 and not held:
            source = start_ref.at[(0, rows - 1)[side], pl.ds(first, width)]
        else:
            source = field.at[(1, rows)[side], pl.ds(first + 1, width), inside]
        return pltpu.make_async_remote_copy(
            src_ref=source,
            dst_ref=field.at[(rows + 1, 0)[side], pl.ds(first + 1, width), inside],
            send_sem=lat_send.at[step % 2, side, chunk],
            recv_sem=lat_recv.at[step % 2, side, chunk],
            device_id={"lat": target},
            device_id_type=MESH,
        )

    def side_copy(step, dim, side, target):
        field = fields[step % 2]
        if dim == 1:
            if step == 0:
                source = start_ref.at[:, (0, columns - 1)[side]]
            else:
                source = field.at[pl.ds(1, rows), (1, columns)[side], inside]
            dest = field.at[pl.ds(1, rows), (columns + 1, 0)[side], inside]
        else:
            if step == 0:
                source = start_ref.at[:, :, pl.ds((0, depth - PAD)[side], PAD)]
            else:
                source = field.at[pl.ds(1, rows), pl.ds(1, columns), pl.ds((PAD, depth)[side], PAD)]
            dest = field.at[pl.ds(1, rows), pl.ds(1, columns), pl.ds((PAD + depth, 0)[side], PAD)]
        return pltpu.make_async_remote_copy(
            src_ref=source,
            dst_ref=dest,
            send_sem=side_send.at[step % 2, dim - 1, side],
            recv_sem=side_recv.at[step % 2, dim - 1, side],
            device_id={AXES[dim]: target},
            device_id_type=MESH,
        )

    def lat_each(step, chunk, act, held=False):
        for side, shift in enumerate((-1, 1)):
            incoming = act == "recv"

            @pl.when(has[0][1 - side if incoming else side])
            def _():
                copy = lat_copy(step, side, chunk, me[0] - shift if incoming else me[0] + shift, held)
                if incoming:
                    copy.wait_recv()
                elif act == "send":
                    copy.wait_send()
                else:
                    copy.start()

    def side_each(step, act):
        for dim in (1, 2):
            for side, shift in enumerate((-1, 1)):
                incoming = act == "recv"

                @pl.when(has[dim][1 - side if incoming else side])
                def _():
                    copy = side_copy(step, dim, side, me[dim] - shift if incoming else me[dim] + shift)
                    if incoming:
                        copy.wait_recv()
                    elif act == "send":
                        copy.wait_send()
                    else:
                        copy.start()

    for load in early:
        load.wait()
    lat_each(0, 0, "start", held=True)

    @pl.loop(1, chunks)
    def _(chunk):
        lat_each(0, chunk, "start")

    side_each(0, "start")
    for load in loads:
        load.start()

    for side in (0, 1):

        @pl.when(jnp.logical_not(has[0][side]))
        def _():
            @pl.loop(1, columns + 1)
            def _(x):
                for field in fields:
                    field[(0, rows + 1)[side], x, inside] = jnp.zeros((depth, lanes), jnp.float32)

        @pl.when(jnp.logical_not(has[1][side]))
        def _():
            for field in fields:
                for y in range(1, rows + 1):
                    field[y, (0, columns + 1)[side], inside] = jnp.zeros((depth, lanes), jnp.float32)

        @pl.when(jnp.logical_not(has[2][side]))
        def _():
            @pl.loop(1, columns + 1)
            def _(x):
                for field in fields:
                    for y in range(1, rows + 1):
                        field[y, x, pl.ds((0, PAD + depth)[side], PAD)] = jnp.zeros((PAD, lanes), jnp.float32)

    for load in loads:
        load.wait()

    outer = (1, rows) if rows > 1 else (1,)
    inner = tuple(range(2, rows))

    for step in range(STEPS):
        now, other = fields[step % 2], fields[(step + 1) % 2]
        last = step == STEPS - 1
        side_each(step, "recv")
        if step > 0:
            side_each(step - 1, "send")

        def advance(y, x):
            middle = now[y, x, inside]
            spread = (
                now[y - 1, x, inside]
                + now[y + 1, x, inside]
                + now[y, x - 1, inside]
                + now[y, x + 1, inside]
                + now[y, x, pl.ds(PAD - 1, depth)]
                + now[y, x, pl.ds(PAD + 1, depth)]
                - 6.0 * middle
            )
            later = 2.0 * middle - other[y, x, inside] + speed[y - 1, x - 1] * spread
            if last:
                end_ref[y - 1, x - 1] = later
            else:
                other[y, x, inside] = later

        @pl.loop(0, chunks)
        def _(chunk):
            def compute(planes):
                if planes:

                    @pl.loop(0, width)
                    def _(offset):
                        for y in planes:
                            advance(y, chunk * width + offset + 1)

            if last:
                compute(inner)
            lat_each(step, chunk, "recv")
            if step > 0:
                lat_each(step - 1, chunk, "send")
            compute(outer)
            if not last:
                compute(inner)
            if not last:
                lat_each(step + 1, chunk, "start")

        if not last:
            side_each(step + 1, "start")

    side_each(STEPS - 1, "send")

    @pl.loop(0, chunks)
    def _(chunk):
        lat_each(STEPS - 1, chunk, "send")


def solution(mesh):
    counts = tuple(mesh.shape[axis] for axis in AXES)

    def shards(pressure, earlier, speed_square):
        rows, columns, depth, lanes = pressure.shape
        chunks = math.gcd(columns, CHUNKS)
        field = pltpu.VMEM((rows + 2, columns + 2, depth + 2 * PAD, lanes), jnp.float32)
        return pl.pallas_call(
            functools.partial(kernel, counts, chunks),
            out_shape=pltpu.VMEM(pressure.shape, jnp.float32),
            in_specs=[pl.BlockSpec(memory_space=pltpu.HBM)] * 3,
            out_specs=pl.BlockSpec(memory_space=pltpu.VMEM),
            scratch_shapes=[
                field,
                field,
                pltpu.VMEM(pressure.shape, jnp.float32),
                pltpu.SemaphoreType.DMA((7,)),
                pltpu.SemaphoreType.DMA((2, 2, chunks)),
                pltpu.SemaphoreType.DMA((2, 2, chunks)),
                pltpu.SemaphoreType.DMA((2, 2, 2)),
                pltpu.SemaphoreType.DMA((2, 2, 2)),
            ],
            compiler_params=pltpu.CompilerParams(
                collective_id=0, has_side_effects=True, vmem_limit_bytes=44 * 2**20
            ),
        )(pressure, earlier, speed_square)

    spec = P("lat", "lon", "lev", None)
    return jax.shard_map(
        shards, mesh=mesh, in_specs=(spec, spec, spec), out_specs=spec, check_vma=False
    )
```
